32 devices in a mesh: seq: 16 (over z, y, x), par: 2 (over core).
Axes of the slice: x: 2, y: 2, z: 4, core: 2. Of those that a mesh axis runs over, the one named last changes fastest.
Arguments:
- states: float32 [4096, 128], P('seq'), may hold values from -6 to 6
- cotangent: float32 [4096, 128], P('seq'), may hold values from -6 to 6
- obs_count: int32 [32], P('seq'), may hold values from 16 to 128
- step_index: int32 [2, 4096], P(None, 'seq'), may hold values from 0 to 15
- step_table: float32 [16], replicated, may hold values from 0.05 to 0.25
- w_in: bfloat16 [128, 2048], P(None, 'par'), may hold values from -0.5 to 0.5
- b_hid: bfloat16 [2048], P('par'), may hold values from -3 to 3
- w_out: bfloat16 [128, 2048], P(None, 'par'), may hold values from -0.125 to 0.125
- b_out: float32 [128], replicated, may hold values from -3 to 3
Outputs:
- state_grad: float32 [4096, 128], P('seq')
- grad_in: float32 [128, 2048], P('seq', 'par')
- grad_out: float32 [128, 2048], P('seq', 'par')
The draws below stay inside these ranges and needn't reach their ends.
All inputs are finite; a program needn't handle non-finite values.
Results may differ from the reference program's by a relative error of at most 0.0055.
Values may be sent and summed in bfloat16 or wider, within the bound.
A program may use at most 64 MiB of HBM per device.

```python
import math
import jax
import jax.numpy as jnp
from jax import lax

L = 128
H = 2048
SLOT = 128
SEQ_DEV = 2
NTAB = 16
SEQS = 32
ROWS = 4096


def plant(array, own_key, low, high):
    longest = array.shape.index(max(array.shape))
    spots = []
    for shift in (0, 1):
        where = [jax.random.randint(jax.random.fold_in(own_key, axis), (), 0, length) for axis, length in enumerate(array.shape)]
        where[longest] = (where[longest] + shift) % array.shape[longest]
        spots.append(tuple(where))
    return array.at[spots[0]].set(low).at[spots[1]].set(high)


def steps_of(stream_key, extent, cuts, smallest, high):
    loudness, own = 1.0, jax.random.fold_in(stream_key, 6)
    for dim, blocks in cuts:
        steps = jnp.exp(jax.random.uniform(jax.random.fold_in(own, dim), (blocks,), jnp.float32, smallest / len(cuts), high / len(cuts)))
        loudness = loudness * jnp.repeat(steps, extent[dim] // blocks).reshape([-1 if axis == dim else 1 for axis in range(len(extent))])
    return loudness


def scatter_about(own_key, dims, width, limit, cuts=(), kind=jnp.bfloat16):
    values = width * jax.random.normal(own_key, dims, jnp.float32)
    if cuts:
        values = values * steps_of(own_key, dims, cuts, -0.22, 0.18)
    return jnp.clip(values, -limit, limit).astype(kind)


def setup_inputs(seed: int = 0) -> dict:
    keys = jax.random.split(jax.random.key(seed), 10)
    return {
        "states": scatter_about(keys[0], (ROWS, L), 1.0, 6.0, ((0, 16),), jnp.float32),
        "cotangent": scatter_about(keys[1], (ROWS, L), 1.0, 6.0, ((0, 16),), jnp.float32),
        "obs_count": plant(jax.random.randint(keys[2], (SEQS,), SLOT // 8, SLOT + 1), jax.random.fold_in(keys[2], 1), SLOT // 8, SLOT).astype(jnp.int32),
        "step_index": plant(jax.random.randint(keys[3], (2, ROWS), 0, NTAB), jax.random.fold_in(keys[3], 1), 0, NTAB - 1).astype(jnp.int32),
        "step_table": jnp.clip(jnp.exp(jax.random.uniform(keys[4], (NTAB,), jnp.float32, math.log(0.05), math.log(0.25))), 0.05, 0.25),
        "w_in": scatter_about(keys[5], (L, H), L ** -0.5, 0.5, ((1, 2),)),
        "b_hid": scatter_about(keys[6], (H,), 0.5, 3.0, ((0, 2),)),
        "w_out": scatter_about(keys[7], (L, H), H ** -0.5, 0.125, ((1, 2),)),
        "b_out": scatter_about(keys[8], (L,), 0.5, 3.0, (), jnp.float32),
    }


COEF_A = [[], [1.0 / 5], [3.0 / 40, 9.0 / 40], [44.0 / 45, -56.0 / 15, 32.0 / 9], [19372.0 / 6561, -25360.0 / 2187, 64448.0 / 6561, -212.0 / 729], [9017.0 / 3168, -355.0 / 33, 46732.0 / 5247, 49.0 / 176, -5103.0 / 18656]]
COEF_B = [35.0 / 384, 0.0, 500.0 / 1113, 125.0 / 192, -2187.0 / 6784, 11.0 / 84]


def identity(value):
    return value


def field(state, w_in, b_hid, w_out, b_out, forward_sum):
    state_b = state.astype(jnp.bfloat16)
    hidden = jnp.tanh(jnp.dot(state_b, w_in, preferred_element_type=jnp.float32) + b_hid.astype(jnp.float32))
    hidden_b = hidden.astype(jnp.bfloat16)
    partial_out = jnp.einsum("rh,lh->rl", hidden_b, w_out, preferred_element_type=jnp.float32)
    return forward_sum(partial_out) + b_out, state_b, hidden, hidden_b


def sweep(states, initial, sizes_list, w_in, b_hid, w_out, b_out, forward_sum, backward_sum):
    value = states
    records = []
    for size_now in sizes_list:
        slopes = []
        saved = []
        for current in range(6):
            if current == 0:
                probe = value
            else:
                combo = COEF_A[current][0] * slopes[0]
                for previous in range(1, current):
                    combo = combo + COEF_A[current][previous] * slopes[previous]
                probe = value + size_now * combo
            slope, state_b, hidden, hidden_b = field(probe, w_in, b_hid, w_out, b_out, forward_sum)
            slopes.append(slope)
            saved.append((state_b, hidden, hidden_b))
        combo = COEF_B[0] * slopes[0]
        for current in range(2, 6):
            combo = combo + COEF_B[current] * slopes[current]
        value = value + size_now * combo
        records.append((size_now, saved))
    back = initial
    grad_in = jnp.zeros(w_in.shape, jnp.float32)
    grad_out = jnp.zeros(w_out.shape, jnp.float32)
    for size_now, saved in reversed(records):
        adjoints = [None] * 6
        total = back
        for current in reversed(range(6)):
            combo = COEF_B[current] * back
            for later in range(current + 1, 6):
                combo = combo + COEF_A[later][current] * adjoints[later]
            grad_b = (size_now * combo).astype(jnp.bfloat16)
            state_b, hidden, hidden_b = saved[current]
            inner = jnp.dot(grad_b, w_out, preferred_element_type=jnp.float32) * (1.0 - hidden * hidden)
            inner_b = inner.astype(jnp.bfloat16)
            partial_back = jnp.einsum("rh,lh->rl", inner_b, w_in, preferred_element_type=jnp.float32)
            adjoints[current] = backward_sum(partial_back)
            total = total + adjoints[current]
            grad_in = grad_in + jnp.einsum("rl,rh->lh", state_b, inner_b, preferred_element_type=jnp.float32)
            grad_out = grad_out + jnp.einsum("rl,rh->lh", grad_b, hidden_b, preferred_element_type=jnp.float32)
        back = total
    return back, grad_in, grad_out


def reference(states, cotangent, obs_count, step_index, step_table, w_in, b_hid, w_out, b_out):
    rows_all = states.shape[0]
    live = (jnp.arange(rows_all, dtype=jnp.int32) % SLOT) < jnp.repeat(obs_count, SLOT)
    initial = cotangent * live[:, None].astype(jnp.float32)
    first_size = step_table[step_index[0]][:, None]
    second_size = step_table[step_index[1]][:, None]
    block = SEQ_DEV * SLOT
    blocks = rows_all // block

    def one_block(carry, pieces):
        block_states, block_initial, size_first, size_second = pieces
        back, grad_in, grad_out = sweep(block_states, block_initial, (size_first, size_second), w_in, b_hid, w_out, b_out, identity, identity)
        return (carry[0] + grad_in, carry[1] + grad_out), back

    zeros = jnp.zeros(w_in.shape, jnp.float32)
    totals, backs = lax.scan(one_block, (zeros, zeros), (states.reshape(blocks, block, -1), initial.reshape(blocks, block, -1), first_size.reshape(blocks, block, 1), second_size.reshape(blocks, block, 1)))
    return backs.reshape(rows_all, -1), totals[0], totals[1]
```

```python
import functools

import jax
import jax.numpy as jnp
from jax import lax
from jax.experimental import pallas as pl
from jax.experimental.pallas import tpu as pltpu
from jax.sharding import PartitionSpec as P

COEF_A = [
    [],
    [1.0 / 5],
    [3.0 / 40, 9.0 / 40],
    [44.0 / 45, -56.0 / 15, 32.0 / 9],
    [19372.0 / 6561, -25360.0 / 2187, 64448.0 / 6561, -212.0 / 729],
    [9017.0 / 3168, -355.0 / 33, 46732.0 / 5247, 49.0 / 176, -5103.0 / 18656],
]
COEF_B = [35.0 / 384, 0.0, 500.0 / 1113, 125.0 / 192, -2187.0 / 6784, 11.0 / 84]
STAGES = 6
STEPS = 2
MESH = pl.DeviceIdType.MESH
F32 = jnp.float32
BF16 = jnp.bfloat16
FIELD_COLS = 512
GRAD_COLS = 512


def dot(a, b):
    return jnp.dot(a, b, preferred_element_type=F32)


def weighted(coefs, values):
    total = None
    for coef, value in zip(coefs, values):
        if coef != 0.0:
            term = coef * value
            total = term if total is None else total + term
    return total


def divisor(total, want):
    size = min(total, want)
    while total % size:
        size -= 128
    return size


class Plan:
    def __init__(self, n_seq, n_par, rows, lat, hid_local):
        self.n_seq, self.n_par = n_seq, n_par
        self.half = rows // n_par
        self.lat, self.hid_local = lat, hid_local
        self.field_cols = divisor(hid_local, FIELD_COLS)
        self.cols = divisor(hid_local, GRAD_COLS)
        self.per_grad = hid_local // self.cols
        self.chunks = 2 * self.per_grad
        self.bits = n_seq.bit_length() - 1
        self.piece = lat // n_seq
        self.scatter = n_seq > 1 and n_seq == 1 << self.bits and lat % (8 * n_seq) == 0
        low = tuple(range(self.bits // 2))
        high = tuple(range(self.bits // 2, self.bits))
        self.orders = []
        if self.scatter:
            for chunk in range(self.chunks):
                order = (high, low) if chunk == 0 else (low, high)
                self.orders.append([group for group in order if group])

    def masks(self, group):
        found = []
        for code in range(1, 1 << len(group)):
            found.append(tuple(bit for place, bit in enumerate(group) if code >> place & 1))
        return found


def kernel(
    plan,
    states,
    cotangent,
    obs_count,
    step_index,
    step_table,
    w_in,
    b_hid,
    w_out,
    b_out,
    *rest,
):
    out_back, out_in, out_out = rest[:3]
    (
        win, wout, bias, win_t, wout_t, sizes, hid, hid_b, inner_b, vb_t, gb_t,
        give, take, own,
        weight_sems, give_sems, back_sems,
    ) = rest[3:20]
    stage_refs = rest[20:]
    n_par, half, hl, cols = plan.n_par, plan.half, plan.hid_local, plan.cols
    par = lax.axis_index("par")
    seq = lax.axis_index("seq")
    bit_of = [(seq // (1 << b)) % 2 for b in range(plan.bits)]

    def across(mask):
        partner = seq
        for b in mask:
            partner = partner + (1 - 2 * bit_of[b]) * (1 << b)
        return partner

    peers = [lax.rem(par + k, n_par) for k in range(n_par)]
    barrier = pltpu.get_barrier_semaphore()
    greeted = 0
    for k in range(1, n_par):
        pl.semaphore_signal(barrier, inc=1, device_id={"par": peers[k]}, device_id_type=MESH)
        greeted += 1
    if plan.scatter:
        for group in plan.orders[0]:
            for mask in plan.masks(group):
                pl.semaphore_signal(
                    barrier, inc=1, device_id={"seq": across(mask)}, device_id_type=MESH
                )
                greeted += 1

    start = par * half
    rows_here = pl.ds(pl.multiple_of(start, 128), half)
    index = step_index[:, rows_here]
    size_rows = jnp.zeros(index.shape, F32)
    for entry in range(step_table.shape[0]):
        size_rows = jnp.where(index == entry, step_table[entry], size_rows)
    for step in range(STEPS):
        spread = jnp.broadcast_to(size_rows[step : step + 1], (plan.lat, half))
        sizes[step] = spread.T
    local_seqs = obs_count.shape[0]
    slot = states.shape[0] // local_seqs
    row = start + lax.broadcasted_iota(jnp.int32, (half, plan.lat), 0)
    live = jnp.zeros((half, plan.lat), F32)
    for one in range(local_seqs):
        first = one * slot
        inside = (row >= first) & (row < first + obs_count[one])
        live = jnp.where(inside, 1.0, live)

    def copies_of_weights():
        made = []
        for k in range(1, n_par):
            for which, (src, dst) in enumerate(
                ((w_in, win), (w_out, wout), (b_hid, bias))
            ):
                made.append(
                    pltpu.make_async_remote_copy(
                        src_ref=src,
                        dst_ref=dst.at[n_par - k - 1],
                        send_sem=weight_sems.at[0, k - 1, which],
                        recv_sem=weight_sems.at[1, n_par - k - 1, which],
                        device_id={"par": peers[k]},
                        device_id_type=MESH,
                    )
                )
        return made

    def transposed(k, in_ref, out_ref):
        win_t[k * hl : (k + 1) * hl, :] = in_ref[...].T
        wout_t[k * hl : (k + 1) * hl, :] = out_ref[...].T

    pl.semaphore_wait(barrier, greeted)
    weights = copies_of_weights()
    for copy in weights:
        copy.start()
    transposed(0, w_in, w_out)
    for copy in weights:
        copy.wait()
    for k in range(1, n_par):
        transposed(k, win.at[k - 1], wout.at[k - 1])

    def pieces():
        for k in range(n_par):
            for c in range(0, hl, plan.field_cols):
                here = slice(c, c + plan.field_cols)
                there = slice(k * hl + c, k * hl + c + plan.field_cols)
                yield k, here, there

    def w_in_at(k, here):
        return w_in[:, here] if k == 0 else win[k - 1, :, here]

    def w_out_at(k, here):
        return w_out[:, here] if k == 0 else wout[k - 1, :, here]

    def bias_at(k, here):
        return b_hid[:, here] if k == 0 else bias[k - 1, :, here]

    def forward(step, value):
        size = sizes[step]
        slopes = []
        for current in range(STAGES):
            at = step * STAGES + current
            probe = value
            if current:
                probe = value + size * weighted(COEF_A[current], slopes)
            state_b = probe.astype(BF16)
            vb_t[at] = state_b.T
            slope = jnp.broadcast_to(b_out[...], (half, plan.lat))
            for k, here, there in pieces():
                hidden = jnp.tanh(dot(state_b, w_in_at(k, here)) + bias_at(k, here))
                hidden_b = hidden.astype(BF16)
                hid[at, :, there] = 1.0 - hidden * hidden
                hid_b[at, :, there] = hidden_b
                slope = slope + dot(hidden_b, wout_t[there, :])
            slopes.append(slope)
        return value + size * weighted(COEF_B, slopes)

    lax.fori_loop(0, STEPS, forward, states[rows_here, :])

    def backward(turn, back):
        step = STEPS - 1 - turn
        size = sizes[step]
        adjoints = [None] * STAGES
        total = back
        for current in reversed(range(STAGES)):
            at = step * STAGES + current
            coefs = [COEF_B[current]] + [
                COEF_A[later][current] for later in range(current + 1, STAGES)
            ]
            grad_b = (size * weighted(coefs, [back] + adjoints[current + 1 :])).astype(BF16)
            gb_t[at] = grad_b.T
            adjoint = None
            for k, here, there in pieces():
                inner = (dot(grad_b, w_out_at(k, here)) * hid[at, :, there]).astype(BF16)
                inner_b[at, :, there] = inner
                part = dot(inner, win_t[there, :])
                adjoint = part if adjoint is None else adjoint + part
            adjoints[current] = adjoint
            total = total + adjoint
        return total

    initial = cotangent[rows_here, :] * live
    out_back[rows_here, :] = lax.fori_loop(0, STEPS, backward, initial)

    def gradient(k, chunk):
        left, right = (vb_t, inner_b) if chunk < plan.per_grad else (gb_t, hid_b)
        begin = k * hl + (chunk % plan.per_grad) * cols
        lhs = jnp.concatenate([left[at] for at in range(STEPS * STAGES)], axis=1)
        rhs = right[:, :, begin : begin + cols].reshape(STEPS * STAGES * half, cols)
        return dot(lhs, rhs)

    waiting = []
    given = {}
    for k in range(1, n_par):
        for chunk in range(plan.chunks):
            give[k - 1, chunk] = gradient(k, chunk).astype(BF16)
            copy = pltpu.make_async_remote_copy(
                src_ref=give.at[k - 1, chunk],
                dst_ref=take.at[n_par - k - 1, chunk],
                send_sem=give_sems.at[0, k - 1, chunk],
                recv_sem=give_sems.at[1, n_par - k - 1, chunk],
                device_id={"par": peers[k]},
                device_id_type=MESH,
            )
            copy.start()
            given[n_par - k - 1, chunk] = copy
            waiting.append(copy)
    back_copies = []
    for k in range(1, n_par):
        copy = pltpu.make_async_remote_copy(
            src_ref=out_back.at[rows_here, :],
            dst_ref=out_back.at[rows_here, :],
            send_sem=back_sems.at[0, k - 1],
            recv_sem=back_sems.at[1, n_par - k - 1],
            device_id={"par": peers[k]},
            device_id_type=MESH,
        )
        copy.start()
        back_copies.append(copy)

    def target(chunk):
        ref = out_in if chunk < plan.per_grad else out_out
        begin = (chunk % plan.per_grad) * cols
        return ref, slice(begin, begin + cols)

    flights = {}

    def launch(chunk, stage):
        send, land, sems = stage_refs[3 * stage : 3 * stage + 3]
        group = plan.orders[chunk][stage]
        left = [b for b in reversed(range(plan.bits)) if b not in sum(plan.orders[chunk][:stage], ())]
        for place, mask in enumerate(plan.masks(group)):
            where = tuple(
                (1 - bit_of[b] if b in mask else bit_of[b]) if b in group else slice(None)
                for b in left
            )
            copy = pltpu.make_async_remote_copy(
                src_ref=send.at[(chunk,) + where],
                dst_ref=land.at[chunk, place],
                send_sem=sems.at[0, chunk, place],
                recv_sem=sems.at[1, chunk, place],
                device_id={"seq": across(mask)},
                device_id_type=MESH,
            )
            copy.start()
            flights.setdefault((chunk, stage), []).append(copy)
            waiting.append(copy)

    for chunk in range(plan.chunks):
        total = gradient(0, chunk)
        for k in range(1, n_par):
            given[k - 1, chunk].wait_recv()
            total = total + take[k - 1, chunk].astype(F32)
        if plan.scatter:
            total = total.reshape((2,) * plan.bits + (plan.piece, cols))
            own[chunk] = total
            stage_refs[0][chunk] = total.astype(BF16)
            launch(chunk, 0)
        else:
            ref, columns = target(chunk)
            ref[:, columns] = total

    if plan.scatter:
        kept = {}
        levels = len(plan.orders[0])
        for stage in range(levels):
            land = stage_refs[3 * stage + 1]
            for chunk in range(plan.chunks):
                group = plan.orders[chunk][stage]
                left = [b for b in reversed(range(plan.bits)) if b not in sum(plan.orders[chunk][:stage], ())]
                where = tuple(bit_of[b] if b in group else slice(None) for b in left)
                total = own[(chunk,) + where] if stage == 0 else kept[chunk].at_own(where)
                for place, copy in enumerate(flights[chunk, stage]):
                    copy.wait_recv()
                    total = total + land[chunk, place].astype(F32)
                if stage == levels - 1:
                    ref, columns = target(chunk)
                    ref[:, columns] = total
                else:
                    own_next = stage_refs[-1]
                    own_next[chunk] = total
                    stage_refs[3 * (stage + 1)][chunk] = total.astype(BF16)
                    kept[chunk] = Kept(own_next, chunk)
                    launch(chunk, stage + 1)

    for copy in waiting:
        copy.wait_send()
    for chunk in given.values() if not plan.scatter else ():
        pass
    for copy in back_copies:
        copy.wait()


class Kept:
    def __init__(self, ref, chunk):
        self.ref, self.chunk = ref, chunk

    def at_own(self, where):
        return self.ref[(self.chunk,) + where]


def per_device(
    states, cotangent, obs_count, step_index, step_table, w_in, b_hid, w_out, b_out
):
    n_seq, n_par = lax.axis_size("seq"), lax.axis_size("par")
    rows, lat = states.shape
    hl = w_in.shape[1]
    plan = Plan(n_seq, n_par, rows, lat, hl)
    half, hidden, sections = plan.half, hl * n_par, STEPS * STAGES
    others = max(n_par - 1, 1)
    vmem = pltpu.VMEM
    dma = pltpu.SemaphoreType.DMA
    scratch = [
        vmem((others, lat, hl), BF16),
        vmem((others, lat, hl), BF16),
        vmem((others, 1, hl), F32),
        vmem((hidden, lat), BF16),
        vmem((hidden, lat), BF16),
        vmem((STEPS, half, lat), F32),
        vmem((sections, half, hidden), F32),
        vmem((sections, half, hidden), BF16),
        vmem((sections, half, hidden), BF16),
        vmem((sections, lat, half), BF16),
        vmem((sections, lat, half), BF16),
        vmem((others, plan.chunks, lat, plan.cols), BF16),
        vmem((others, plan.chunks, lat, plan.cols), BF16),
        vmem(
            (plan.chunks,) + ((2,) * plan.bits + (plan.piece, plan.cols) if plan.scatter else (8, 128)),
            F32,
        ),
        dma((2, others, 3)),
        dma((2, others, plan.chunks)),
        dma((2, others)),
    ]
    grad_rows = plan.piece if plan.scatter else lat
    if plan.scatter:
        left = plan.bits
        for group_size in [len(group) for group in plan.orders[0]]:
            tail = (plan.piece, plan.cols)
            masks = (1 << group_size) - 1
            scratch.append(vmem((plan.chunks,) + (2,) * left + tail, BF16))
            left -= group_size
            scratch.append(vmem((plan.chunks, masks) + (2,) * left + tail, BF16))
            scratch.append(dma((2, plan.chunks, masks)))
        middle = plan.bits - len(plan.orders[0][0])
        scratch.append(vmem((plan.chunks,) + (2,) * middle + (plan.piece, plan.cols), F32))
    in_vmem = pl.BlockSpec(memory_space=pltpu.VMEM)
    in_smem = pl.BlockSpec(memory_space=pltpu.SMEM)
    back, grad_in, grad_out = pl.pallas_call(
        functools.partial(kernel, plan),
        name="adjoint",
        out_shape=(
            jax.ShapeDtypeStruct((rows, lat), F32),
            jax.ShapeDtypeStruct((grad_rows, hl), F32),
            jax.ShapeDtypeStruct((grad_rows, hl), F32),
        ),
        in_specs=[in_vmem, in_vmem, in_smem, in_vmem, in_smem] + [in_vmem] * 4,
        out_specs=(in_vmem,) * 3,
        scratch_shapes=scratch,
        compiler_params=pltpu.CompilerParams(
            collective_id=0,
            has_side_effects=True,
            vmem_limit_bytes=60 * 1024 * 1024,
        ),
    )(
        states,
        cotangent,
        obs_count,
        step_index,
        step_table,
        w_in,
        b_hid.astype(F32)[None, :],
        w_out,
        b_out[None, :],
    )
    if not plan.scatter:
        grad_in, grad_out = (
            lax.psum_scatter(grad, "seq", scatter_dimension=0, tiled=True)
            for grad in (grad_in, grad_out)
        )
    return (back, grad_in, grad_out)


def solution(mesh):
    return jax.shard_map(
        per_device,
        mesh=mesh,
        in_specs=(
            P("seq", None),
            P("seq", None),
            P("seq"),
            P(None, "seq"),
            P(),
            P(None, "par"),
            P("par"),
            P(None, "par"),
            P(),
        ),
        out_specs=(P("seq", None), P("seq", "par"), P("seq", "par")),
        check_vma=False,
    )
```

```python
import functools

import jax
import jax.numpy as jnp
from jax import lax
from jax.experimental import pallas as pl
from jax.experimental.pallas import tpu as pltpu
from jax.sharding import PartitionSpec as P

COEF_A = [
    [],
    [1.0 / 5],
    [3.0 / 40, 9.0 / 40],
    [44.0 / 45, -56.0 / 15, 32.0 / 9],
    [19372.0 / 6561, -25360.0 / 2187, 64448.0 / 6561, -212.0 / 729],
    [9017.0 / 3168, -355.0 / 33, 46732.0 / 5247, 49.0 / 176, -5103.0 / 18656],
]
COEF_B = [35.0 / 384, 0.0, 500.0 / 1113, 125.0 / 192, -2187.0 / 6784, 11.0 / 84]
STAGES = 6
STEPS = 2
MESH = pl.DeviceIdType.MESH
F32 = jnp.float32
BF16 = jnp.bfloat16
FIELD_COLS = 512
GRAD_COLS = 512


def dot(a, b):
    return jnp.dot(a, b, preferred_element_type=F32)


def weighted(coefs, values):
    total = None
    for coef, value in zip(coefs, values):
        if coef != 0.0:
            term = coef * value
            total = term if total is None else total + term
    return total


def divisor(total, want):
    size = min(total, want)
    while total % size:
        size -= 128
    return size


def orders_of(chunk, low, high):
    return (high, low) if chunk == 0 else (low, high)


class Plan:
    def __init__(self, n_seq, n_par, rows, lat, hid_local):
        self.n_seq, self.n_par = n_seq, n_par
        self.half = rows // n_par
        self.lat, self.hid_local = lat, hid_local
        self.field_cols = divisor(hid_local, FIELD_COLS)
        self.cols = divisor(hid_local, GRAD_COLS)
        self.per_grad = hid_local // self.cols
        self.chunks = 2 * self.per_grad
        self.bits = n_seq.bit_length() - 1
        self.piece = lat // n_seq
        self.scatter = n_seq > 1 and n_seq == 1 << self.bits and lat % (8 * n_seq) == 0
        low = tuple(range(self.bits // 2))
        high = tuple(range(self.bits // 2, self.bits))
        self.orders = []
        self.base = []
        self.messages = 0
        if self.scatter:
            for chunk in range(self.chunks):
                order = orders_of(chunk, low, high)
                self.orders.append([group for group in order if group])
                self.base.append([])
                for group in self.orders[-1]:
                    self.base[-1].append(self.messages)
                    self.messages += (1 << len(group)) - 1

    def left(self, chunk, stage):
        gone = sum(self.orders[chunk][:stage], ())
        return [b for b in reversed(range(self.bits)) if b not in gone]

    def partners(self):
        found = set()
        for order in self.orders:
            for group in order:
                found.update(self.masks(group))
        return sorted(found)

    def masks(self, group):
        found = []
        for code in range(1, 1 << len(group)):
            found.append(tuple(bit for place, bit in enumerate(group) if code >> place & 1))
        return found


def kernel(
    plan,
    states_h,
    cotangent_h,
    obs_count_h,
    step_index_h,
    step_table_h,
    w_in_h,
    b_hid_h,
    w_out_h,
    b_out_h,
    *rest,
):
    out_back, out_in, out_out = rest[:3]
    (
        states, cotangent, obs_count, step_index, step_table, w_in, b_hid, w_out, b_out,
        local_sems,
        win, wout, bias, win_t, wout_t, sizes, hid, hid_b, inner_b, vb_t, gb_t,
        give, take,
        weight_sems, give_sems, back_sems,
    ) = rest[3:29]
    stage_refs = rest[29:]
    if plan.scatter:
        seq_sems = stage_refs[0]
        stage_refs = stage_refs[1:]
    n_par, half, hl, cols = plan.n_par, plan.half, plan.hid_local, plan.cols
    par = lax.axis_index("par")
    seq = lax.axis_index("seq")
    bit_of = [(seq // (1 << b)) % 2 for b in range(plan.bits)]
    start = par * half
    rows_here = pl.ds(pl.multiple_of(start, 128), half)

    loads = {}
    for place, (name, src, dst) in enumerate(
        (
            ("w_in", w_in_h, w_in),
            ("w_out", w_out_h, w_out),
            ("b_hid", b_hid_h, b_hid),
            ("step_index", step_index_h, step_index),
            ("step_table", step_table_h, step_table),
            ("states", states_h.at[rows_here, :], states),
            ("b_out", b_out_h, b_out),
            ("cotangent", cotangent_h.at[rows_here, :], cotangent),
            ("obs_count", obs_count_h, obs_count),
        )
    ):
        loads[name] = pltpu.make_async_copy(src, dst, local_sems.at[place])
        loads[name].start()

    def across(mask):
        partner = seq
        for b in mask:
            partner = partner + (1 - 2 * bit_of[b]) * (1 << b)
        return partner

    peers = [lax.rem(par + k, n_par) for k in range(n_par)]
    barrier = pltpu.get_barrier_semaphore()
    greeted = 0
    for mask in plan.partners():
        pl.semaphore_signal(barrier, inc=1, device_id={"seq": across(mask)}, device_id_type=MESH)
        greeted += 1
    for k in range(1, n_par):
        pl.semaphore_signal(barrier, inc=1, device_id={"par": peers[k]}, device_id_type=MESH)
        greeted += 1

    def transposed(k, in_ref, out_ref):
        win_t[k * hl : (k + 1) * hl, :] = in_ref[...].T
        wout_t[k * hl : (k + 1) * hl, :] = out_ref[...].T

    for name in ("w_in", "w_out", "b_hid"):
        loads[name].wait()

    def copies_of_weights():
        made = []
        for k in range(1, n_par):
            for which, (src, dst) in enumerate(
                ((w_in, win), (w_out, wout), (b_hid, bias))
            ):
                made.append(
                    pltpu.make_async_remote_copy(
                        src_ref=src,
                        dst_ref=dst.at[n_par - k - 1],
                        send_sem=weight_sems.at[0, k - 1, which],
                        recv_sem=weight_sems.at[1, n_par - k - 1, which],
                        device_id={"par": peers[k]},
                        device_id_type=MESH,
                    )
                )
        return made

    if greeted:
        pl.semaphore_wait(barrier, greeted)
    weights = copies_of_weights()
    for copy in weights:
        copy.start()
    transposed(0, w_in, w_out)
    for name in ("step_index", "step_table", "states", "b_out", "cotangent", "obs_count"):
        loads[name].wait()

    index = step_index[:, rows_here]
    size_rows = jnp.zeros(index.shape, F32)
    for entry in range(step_table.shape[0]):
        size_rows = jnp.where(index == entry, step_table[entry], size_rows)
    for step in range(STEPS):
        spread = jnp.broadcast_to(size_rows[step : step + 1], (plan.lat, half))
        sizes[step] = spread.T
    local_seqs = obs_count.shape[0]
    slot = states_h.shape[0] // local_seqs
    row = start + lax.broadcasted_iota(jnp.int32, (half, plan.lat), 0)
    live = jnp.zeros((half, plan.lat), F32)
    for one in range(local_seqs):
        first = one * slot
        inside = (row >= first) & (row < first + obs_count[one])
        live = jnp.where(inside, 1.0, live)

    for copy in weights:
        copy.wait()
    for k in range(1, n_par):
        transposed(k, win.at[k - 1], wout.at[k - 1])

    def pieces():
        for k in range(n_par):
            for c in range(0, hl, plan.field_cols):
                here = slice(c, c + plan.field_cols)
                there = slice(k * hl + c, k * hl + c + plan.field_cols)
                yield k, here, there

    def w_in_at(k, here):
        return w_in[:, here] if k == 0 else win[k - 1, :, here]

    def w_out_at(k, here):
        return w_out[:, here] if k == 0 else wout[k - 1, :, here]

    def bias_at(k, here):
        return b_hid[:, here] if k == 0 else bias[k - 1, :, here]

    def forward(step, value):
        size = sizes[step]
        slopes = []
        for current in range(STAGES):
            at = step * STAGES + current
            probe = value
            if current:
                probe = value + size * weighted(COEF_A[current], slopes)
            state_b = probe.astype(BF16)
            vb_t[at] = state_b.T
            slope = jnp.broadcast_to(b_out[...], (half, plan.lat))
            for k, here, there in pieces():
                hidden = jnp.tanh(dot(state_b, w_in_at(k, here)) + bias_at(k, here))
                hid[at, :, there] = 1.0 - hidden * hidden
                hid_b[at, :, there] = hidden.astype(BF16)
            slope = slope + dot(hid_b[at], wout_t[...])
            slopes.append(slope)
        return value + size * weighted(COEF_B, slopes)

    lax.fori_loop(0, STEPS, forward, states[...])

    def backward(turn, back):
        step = STEPS - 1 - turn
        size = sizes[step]
        adjoints = [None] * STAGES
        total = back
        for current in reversed(range(STAGES)):
            at = step * STAGES + current
            coefs = [COEF_B[current]] + [
                COEF_A[later][current] for later in range(current + 1, STAGES)
            ]
            grad_b = (size * weighted(coefs, [back] + adjoints[current + 1 :])).astype(BF16)
            gb_t[at] = grad_b.T
            for k, here, there in pieces():
                inner = dot(grad_b, w_out_at(k, here)) * hid[at, :, there]
                inner_b[at, :, there] = inner.astype(BF16)
            adjoint = dot(inner_b[at], win_t[...])
            adjoints[current] = adjoint
            total = total + adjoint
        return total

    initial = cotangent[...] * live
    out_back[rows_here, :] = lax.fori_loop(0, STEPS, backward, initial)

    def gradient(k, chunk):
        left, right = (vb_t, inner_b) if chunk < plan.per_grad else (gb_t, hid_b)
        begin = k * hl + (chunk % plan.per_grad) * cols
        lhs = jnp.concatenate([left[at] for at in range(STEPS * STAGES)], axis=1)
        rhs = right[:, :, begin : begin + cols].reshape(STEPS * STAGES * half, cols)
        return dot(lhs, rhs)

    waiting = []
    given = {}
    for k in range(1, n_par):
        for chunk in range(plan.chunks):
            give[k - 1, chunk] = gradient(k, chunk).astype(BF16)
            copy = pltpu.make_async_remote_copy(
                src_ref=give.at[k - 1, chunk],
                dst_ref=take.at[n_par - k - 1, chunk],
                send_sem=give_sems.at[0, k - 1, chunk],
                recv_sem=give_sems.at[1, n_par - k - 1, chunk],
                device_id={"par": peers[k]},
                device_id_type=MESH,
            )
            copy.start()
            given[n_par - k - 1, chunk] = copy
            waiting.append(copy)
    back_copies = []
    for k in range(1, n_par):
        copy = pltpu.make_async_remote_copy(
            src_ref=out_back.at[rows_here, :],
            dst_ref=out_back.at[rows_here, :],
            send_sem=back_sems.at[0, k - 1],
            recv_sem=back_sems.at[1, n_par - k - 1],
            device_id={"par": peers[k]},
            device_id_type=MESH,
        )
        copy.start()
        back_copies.append(copy)

    def target(chunk):
        ref = out_in if chunk < plan.per_grad else out_out
        begin = (chunk % plan.per_grad) * cols
        return ref, slice(begin, begin + cols)

    refs = {}
    if plan.scatter:
        count = 0
        for chunk in range(plan.chunks):
            for stage in range(len(plan.orders[chunk])):
                refs[chunk, stage] = stage_refs[count : count + 3]
                count += 3
    flights = {}

    def launch(chunk, stage, total):
        keep, send, land = refs[chunk, stage]
        keep[...] = total
        send[...] = total.astype(BF16)
        group = plan.orders[chunk][stage]
        left = plan.left(chunk, stage)
        flights[chunk, stage] = []
        for place, mask in enumerate(plan.masks(group)):
            where = tuple(
                (1 - bit_of[b] if b in mask else bit_of[b]) if b in group else slice(None)
                for b in left
            )
            number = plan.base[chunk][stage] + place
            copy = pltpu.make_async_remote_copy(
                src_ref=send.at[where],
                dst_ref=land.at[place],
                send_sem=seq_sems.at[0, number],
                recv_sem=seq_sems.at[1, number],
                device_id={"seq": across(mask)},
                device_id_type=MESH,
            )
            copy.start()
            flights[chunk, stage].append(copy)
            waiting.append(copy)

    for chunk in range(plan.chunks):
        total = gradient(0, chunk)
        for k in range(1, n_par):
            given[k - 1, chunk].wait_recv()
            total = total + take[k - 1, chunk].astype(F32)
        if plan.scatter:
            launch(chunk, 0, total.reshape((2,) * plan.bits + (plan.piece, cols)))
        else:
            ref, columns = target(chunk)
            ref[:, columns] = total

    if plan.scatter:
        for stage in range(max(len(order) for order in plan.orders)):
            for chunk in range(plan.chunks):
                if stage >= len(plan.orders[chunk]):
                    continue
                keep, _, land = refs[chunk, stage]
                group = plan.orders[chunk][stage]
                where = tuple(
                    bit_of[b] if b in group else slice(None) for b in plan.left(chunk, stage)
                )
                total = keep[where]
                for place, copy in enumerate(flights[chunk, stage]):
                    copy.wait_recv()
                    total = total + land[place].astype(F32)
                if stage == len(plan.orders[chunk]) - 1:
                    ref, columns = target(chunk)
                    ref[:, columns] = total
                else:
                    launch(chunk, stage + 1, total)

    for copy in waiting:
        copy.wait_send()
    for copy in back_copies:
        copy.wait()


def per_device(
    states, cotangent, obs_count, step_index, step_table, w_in, b_hid, w_out, b_out
):
    n_seq, n_par = lax.axis_size("seq"), lax.axis_size("par")
    rows, lat = states.shape
    hl = w_in.shape[1]
    plan = Plan(n_seq, n_par, rows, lat, hl)
    half, hidden, sections = plan.half, hl * n_par, STEPS * STAGES
    others = max(n_par - 1, 1)
    vmem = pltpu.VMEM
    dma = pltpu.SemaphoreType.DMA
    scratch = [
        vmem((half, lat), F32),
        vmem((half, lat), F32),
        pltpu.SMEM(obs_count.shape, obs_count.dtype),
        vmem(step_index.shape, step_index.dtype),
        pltpu.SMEM(step_table.shape, F32),
        vmem((lat, hl), BF16),
        vmem((1, hl), F32),
        vmem((lat, hl), BF16),
        vmem((1, lat), F32),
        dma((9,)),
        vmem((others, lat, hl), BF16),
        vmem((others, lat, hl), BF16),
        vmem((others, 1, hl), F32),
        vmem((hidden, lat), BF16),
        vmem((hidden, lat), BF16),
        vmem((STEPS, half, lat), F32),
        vmem((sections, half, hidden), F32),
        vmem((sections, half, hidden), BF16),
        vmem((sections, half, hidden), BF16),
        vmem((sections, lat, half), BF16),
        vmem((sections, lat, half), BF16),
        vmem((others, plan.chunks, lat, plan.cols), BF16),
        vmem((others, plan.chunks, lat, plan.cols), BF16),
        dma((2, others, 3)),
        dma((2, others, plan.chunks)),
        dma((2, others)),
    ]
    grad_rows = plan.piece if plan.scatter else lat
    if plan.scatter:
        scratch.append(dma((2, plan.messages)))
        tail = (plan.piece, plan.cols)
        for chunk in range(plan.chunks):
            for stage, group in enumerate(plan.orders[chunk]):
                here = (2,) * len(plan.left(chunk, stage)) + tail
                after = (2,) * len(plan.left(chunk, stage + 1)) + tail
                scratch.append(vmem(here, F32))
                scratch.append(vmem(here, BF16))
                scratch.append(vmem(((1 << len(group)) - 1,) + after, BF16))
    in_vmem = pl.BlockSpec(memory_space=pltpu.VMEM)
    anywhere = pl.BlockSpec(memory_space=pl.ANY)
    back, grad_in, grad_out = pl.pallas_call(
        functools.partial(kernel, plan),
        name="adjoint",
        out_shape=(
            jax.ShapeDtypeStruct((rows, lat), F32),
            jax.ShapeDtypeStruct((grad_rows, hl), F32),
            jax.ShapeDtypeStruct((grad_rows, hl), F32),
        ),
        in_specs=[anywhere] * 9,
        out_specs=(in_vmem,) * 3,
        scratch_shapes=scratch,
        compiler_params=pltpu.CompilerParams(
            collective_id=0,
            has_side_effects=True,
            vmem_limit_bytes=60 * 1024 * 1024,
        ),
    )(
        states,
        cotangent,
        obs_count,
        step_index,
        step_table,
        w_in,
        b_hid.astype(F32)[None, :],
        w_out,
        b_out[None, :],
    )
    if not plan.scatter:
        grad_in, grad_out = (
            lax.psum_scatter(grad, "seq", scatter_dimension=0, tiled=True)
            for grad in (grad_in, grad_out)
        )
    return (back, grad_in, grad_out)


def solution(mesh):
    return jax.shard_map(
        per_device,
        mesh=mesh,
        in_specs=(
            P("seq", None),
            P("seq", None),
            P("seq"),
            P(None, "seq"),
            P(),
            P(None, "par"),
            P("par"),
            P(None, "par"),
            P(),
        ),
        out_specs=(P("seq", None), P("seq", "par"), P("seq", "par")),
        check_vma=False,
    )
```

```python
import functools

import jax
import jax.numpy as jnp
from jax import lax
from jax.experimental import pallas as pl
from jax.experimental.pallas import tpu as pltpu
from jax.sharding import PartitionSpec as P

COEF_A = [
    [],
    [1.0 / 5],
    [3.0 / 40, 9.0 / 40],
    [44.0 / 45, -56.0 / 15, 32.0 / 9],
    [19372.0 / 6561, -25360.0 / 2187, 64448.0 / 6561, -212.0 / 729],
    [9017.0 / 3168, -355.0 / 33, 46732.0 / 5247, 49.0 / 176, -5103.0 / 18656],
]
COEF_B = [35.0 / 384, 0.0, 500.0 / 1113, 125.0 / 192, -2187.0 / 6784, 11.0 / 84]
STAGES = 6
STEPS = 2
MESH = pl.DeviceIdType.MESH
F32 = jnp.float32
BF16 = jnp.bfloat16
FIELD_COLS = 512
GRAD_COLS = 512


def dot(a, b):
    return jnp.dot(a, b, preferred_element_type=F32)


def weighted(coefs, values):
    total = None
    for coef, value in zip(coefs, values):
        if coef != 0.0:
            term = coef * value
            total = term if total is None else total + term
    return total


def divisor(total, want):
    size = min(total, want)
    while total % size:
        size -= 128
    return size


def orders_of(chunk, low, high):
    return (high, low) if chunk == 0 else (low, high)


class Plan:
    def __init__(self, n_seq, n_par, rows, lat, hid_local):
        self.n_seq, self.n_par = n_seq, n_par
        self.half = rows // n_par
        self.lat, self.hid_local = lat, hid_local
        self.field_cols = divisor(hid_local, FIELD_COLS)
        self.cols = divisor(hid_local, GRAD_COLS)
        self.per_grad = hid_local // self.cols
        self.chunks = 2 * self.per_grad
        self.bits = n_seq.bit_length() - 1
        self.piece = lat // n_seq
        self.scatter = n_seq > 1 and n_seq == 1 << self.bits and lat % (8 * n_seq) == 0
        low = tuple(range(self.bits // 2))
        high = tuple(range(self.bits // 2, self.bits))
        self.orders = []
        self.base = []
        self.messages = 0
        if self.scatter:
            for chunk in range(self.chunks):
                order = orders_of(chunk, low, high)
                self.orders.append([group for group in order if group])
                self.base.append([])
                for group in self.orders[-1]:
                    self.base[-1].append(self.messages)
                    self.messages += (1 << len(group)) - 1

    def left(self, chunk, stage):
        gone = sum(self.orders[chunk][:stage], ())
        return [b for b in reversed(range(self.bits)) if b not in gone]

    def partners(self):
        found = set()
        for order in self.orders:
            for group in order:
                found.update(self.masks(group))
        return sorted(found)

    def masks(self, group):
        found = []
        for code in range(1, 1 << len(group)):
            found.append(tuple(bit for place, bit in enumerate(group) if code >> place & 1))
        return found


def kernel(
    plan,
    states_h,
    cotangent_h,
    obs_count_h,
    step_index_h,
    step_table_h,
    w_in_h,
    b_hid_h,
    w_out_h,
    b_out_h,
    *rest,
):
    out_back, out_in, out_out = rest[:3]
    (
        states, cotangent, obs_count, step_index, step_table, w_in, b_hid, w_out, b_out,
        local_sems,
        win, wout, bias, bias_rows, win_t, wout_t, sizes, hid, hid_b, inner_b, vb_t, gb_t,
        give, take,
        weight_sems, give_sems, back_sems,
    ) = rest[3:30]
    stage_refs = rest[30:]
    if plan.scatter:
        seq_sems = stage_refs[0]
        stage_refs = stage_refs[1:]
    n_par, half, hl, cols = plan.n_par, plan.half, plan.hid_local, plan.cols
    par = lax.axis_index("par")
    seq = lax.axis_index("seq")
    bit_of = [(seq // (1 << b)) % 2 for b in range(plan.bits)]
    start = par * half
    rows_here = pl.ds(pl.multiple_of(start, 128), half)

    loads = {}
    for place, (name, src, dst) in enumerate(
        (
            ("w_in", w_in_h, w_in),
            ("w_out", w_out_h, w_out),
            ("b_hid", b_hid_h, b_hid),
            ("step_index", step_index_h, step_index),
            ("step_table", step_table_h, step_table),
            ("states", states_h.at[rows_here, :], states),
            ("b_out", b_out_h, b_out),
            ("cotangent", cotangent_h.at[rows_here, :], cotangent),
            ("obs_count", obs_count_h, obs_count),
        )
    ):
        loads[name] = pltpu.make_async_copy(src, dst, local_sems.at[place])
        loads[name].start()

    def across(mask):
        partner = seq
        for b in mask:
            partner = partner + (1 - 2 * bit_of[b]) * (1 << b)
        return partner

    peers = [lax.rem(par + k, n_par) for k in range(n_par)]
    barrier = pltpu.get_barrier_semaphore()
    greeted = 0
    for mask in plan.partners():
        pl.semaphore_signal(barrier, inc=1, device_id={"seq": across(mask)}, device_id_type=MESH)
        greeted += 1
    for k in range(1, n_par):
        pl.semaphore_signal(barrier, inc=1, device_id={"par": peers[k]}, device_id_type=MESH)
        greeted += 1

    def transposed(k, in_ref, out_ref):
        win_t[k * hl : (k + 1) * hl, :] = in_ref[...].T
        wout_t[k * hl : (k + 1) * hl, :] = out_ref[...].T

    for name in ("w_in", "w_out", "b_hid"):
        loads[name].wait()

    def copies_of_weights():
        made = []
        for k in range(1, n_par):
            for which, (src, dst) in enumerate(
                ((w_in, win), (w_out, wout), (b_hid, bias))
            ):
                made.append(
                    pltpu.make_async_remote_copy(
                        src_ref=src,
                        dst_ref=dst if len(dst.shape) == 1 else dst.at[n_par - k - 1],
                        send_sem=weight_sems.at[0, k - 1, which],
                        recv_sem=weight_sems.at[1, n_par - k - 1, which],
                        device_id={"par": peers[k]},
                        device_id_type=MESH,
                    )
                )
        return made

    if greeted:
        pl.semaphore_wait(barrier, greeted)
    weights = copies_of_weights()
    for copy in weights:
        copy.start()
    transposed(0, w_in, w_out)
    for name in ("step_index", "step_table", "states", "b_out", "cotangent", "obs_count"):
        loads[name].wait()

    index = step_index[:, rows_here]
    size_rows = jnp.zeros(index.shape, F32)
    for entry in range(step_table.shape[0]):
        size_rows = jnp.where(index == entry, step_table[entry], size_rows)
    for step in range(STEPS):
        spread = jnp.broadcast_to(size_rows[step : step + 1], (plan.lat, half))
        sizes[step] = spread.T
    local_seqs = obs_count.shape[0]
    slot = states_h.shape[0] // local_seqs
    row = start + lax.broadcasted_iota(jnp.int32, (half, plan.lat), 0)
    live = jnp.zeros((half, plan.lat), F32)
    for one in range(local_seqs):
        first = one * slot
        inside = (row >= first) & (row < first + obs_count[one])
        live = jnp.where(inside, 1.0, live)

    for copy in weights:
        copy.wait()
    for k in range(1, n_par):
        transposed(k, win.at[k - 1], wout.at[k - 1])

    bias_rows[0:1, :] = b_hid[...].astype(F32).reshape(1, hl)
    for k in range(1, n_par):
        far = bias[...] if len(bias.shape) == 1 else bias[k - 1]
        bias_rows[k : k + 1, :] = far.astype(F32).reshape(1, hl)

    def pieces():
        for k in range(n_par):
            for c in range(0, hl, plan.field_cols):
                here = slice(c, c + plan.field_cols)
                there = slice(k * hl + c, k * hl + c + plan.field_cols)
                yield k, here, there

    def w_in_at(k, here):
        return w_in[:, here] if k == 0 else win[k - 1, :, here]

    def w_out_at(k, here):
        return w_out[:, here] if k == 0 else wout[k - 1, :, here]

    def bias_at(k, here):
        return bias_rows[k : k + 1, here]

    def forward(step, value):
        size = sizes[step]
        slopes = []
        for current in range(STAGES):
            at = step * STAGES + current
            probe = value
            if current:
                probe = value + size * weighted(COEF_A[current], slopes)
            state_b = probe.astype(BF16)
            vb_t[at] = state_b.T
            slope = jnp.broadcast_to(b_out[...], (half, plan.lat))
            for k, here, there in pieces():
                hidden = jnp.tanh(dot(state_b, w_in_at(k, here)) + bias_at(k, here))
                hid[at, :, there] = hidden
                hid_b[at, :, there] = hidden.astype(BF16)
            slope = slope + dot(hid_b[at], wout_t[...])
            slopes.append(slope)
        return value + size * weighted(COEF_B, slopes)

    lax.fori_loop(0, STEPS, forward, states[...])

    def backward(turn, back):
        step = STEPS - 1 - turn
        size = sizes[step]
        adjoints = [None] * STAGES
        total = back
        for current in reversed(range(STAGES)):
            at = step * STAGES + current
            coefs = [COEF_B[current]] + [
                COEF_A[later][current] for later in range(current + 1, STAGES)
            ]
            grad_b = (size * weighted(coefs, [back] + adjoints[current + 1 :])).astype(BF16)
            gb_t[at] = grad_b.T
            for k, here, there in pieces():
                inner = dot(grad_b, w_out_at(k, here)) * (1.0 - hid[at, :, there] * hid[at, :, there])
                inner_b[at, :, there] = inner.astype(BF16)
            adjoint = dot(inner_b[at], win_t[...])
            adjoints[current] = adjoint
            total = total + adjoint
        return total

    initial = cotangent[...] * live
    out_back[rows_here, :] = lax.fori_loop(0, STEPS, backward, initial)

    def gradient(k, chunk):
        left, right = (vb_t, inner_b) if chunk < plan.per_grad else (gb_t, hid_b)
        begin = k * hl + (chunk % plan.per_grad) * cols
        lhs = jnp.concatenate([left[at] for at in range(STEPS * STAGES)], axis=1)
        rhs = right[:, :, begin : begin + cols].reshape(STEPS * STAGES * half, cols)
        return dot(lhs, rhs)

    waiting = []
    given = {}

    def hand_over(chunk):
        for k in range(1, n_par):
            give[k - 1, chunk] = gradient(k, chunk).astype(BF16)
            copy = pltpu.make_async_remote_copy(
                src_ref=give.at[k - 1, chunk],
                dst_ref=take.at[n_par - k - 1, chunk],
                send_sem=give_sems.at[0, k - 1, chunk],
                recv_sem=give_sems.at[1, n_par - k - 1, chunk],
                device_id={"par": peers[k]},
                device_id_type=MESH,
            )
            copy.start()
            given[n_par - k - 1, chunk] = copy
            waiting.append(copy)
    back_copies = []
    for k in range(1, n_par):
        copy = pltpu.make_async_remote_copy(
            src_ref=out_back.at[rows_here, :],
            dst_ref=out_back.at[rows_here, :],
            send_sem=back_sems.at[0, k - 1],
            recv_sem=back_sems.at[1, n_par - k - 1],
            device_id={"par": peers[k]},
            device_id_type=MESH,
        )
        copy.start()
        back_copies.append(copy)

    def target(chunk):
        ref = out_in if chunk < plan.per_grad else out_out
        begin = (chunk % plan.per_grad) * cols
        return ref, slice(begin, begin + cols)

    refs = {}
    if plan.scatter:
        count = 0
        for chunk in range(plan.chunks):
            for stage in range(len(plan.orders[chunk])):
                refs[chunk, stage] = stage_refs[count : count + 3]
                count += 3
    flights = {}

    def launch(chunk, stage, total):
        keep, send, land = refs[chunk, stage]
        keep[...] = total
        send[...] = total.astype(BF16)
        group = plan.orders[chunk][stage]
        left = plan.left(chunk, stage)
        flights[chunk, stage] = []
        for place, mask in enumerate(plan.masks(group)):
            where = tuple(
                (1 - bit_of[b] if b in mask else bit_of[b]) if b in group else slice(None)
                for b in left
            )
            number = plan.base[chunk][stage] + place
            copy = pltpu.make_async_remote_copy(
                src_ref=send.at[where],
                dst_ref=land.at[place],
                send_sem=seq_sems.at[0, number],
                recv_sem=seq_sems.at[1, number],
                device_id={"seq": across(mask)},
                device_id_type=MESH,
            )
            copy.start()
            flights[chunk, stage].append(copy)
            waiting.append(copy)

    hand_over(0)
    for chunk in range(plan.chunks):
        if chunk + 1 < plan.chunks:
            hand_over(chunk + 1)
        total = gradient(0, chunk)
        for k in range(1, n_par):
            given[k - 1, chunk].wait_recv()
            total = total + take[k - 1, chunk].astype(F32)
        if plan.scatter:
            launch(chunk, 0, total.reshape((2,) * plan.bits + (plan.piece, cols)))
        else:
            ref, columns = target(chunk)
            ref[:, columns] = total

    if plan.scatter:
        for stage in range(max(len(order) for order in plan.orders)):
            for chunk in range(plan.chunks):
                if stage >= len(plan.orders[chunk]):
                    continue
                keep, _, land = refs[chunk, stage]
                group = plan.orders[chunk][stage]
                where = tuple(
                    bit_of[b] if b in group else slice(None) for b in plan.left(chunk, stage)
                )
                total = keep[where]
                for place, copy in enumerate(flights[chunk, stage]):
                    copy.wait_recv()
                    total = total + land[place].astype(F32)
                if stage == len(plan.orders[chunk]) - 1:
                    ref, columns = target(chunk)
                    ref[:, columns] = total
                else:
                    launch(chunk, stage + 1, total)

    for copy in waiting:
        copy.wait_send()
    for copy in back_copies:
        copy.wait()


def per_device(
    states, cotangent, obs_count, step_index, step_table, w_in, b_hid, w_out, b_out
):
    n_seq, n_par = lax.axis_size("seq"), lax.axis_size("par")
    rows, lat = states.shape
    hl = w_in.shape[1]
    plan = Plan(n_seq, n_par, rows, lat, hl)
    half, hidden, sections = plan.half, hl * n_par, STEPS * STAGES
    others = max(n_par - 1, 1)
    vmem = pltpu.VMEM
    dma = pltpu.SemaphoreType.DMA
    scratch = [
        vmem((half, lat), F32),
        vmem((half, lat), F32),
        pltpu.SMEM(obs_count.shape, obs_count.dtype),
        vmem(step_index.shape, step_index.dtype),
        pltpu.SMEM(step_table.shape, F32),
        vmem((lat, hl), BF16),
        vmem((hl,), BF16),
        vmem((lat, hl), BF16),
        vmem((1, lat), F32),
        dma((9,)),
        vmem((others, lat, hl), BF16),
        vmem((others, lat, hl), BF16),
        vmem((others, hl), BF16) if n_par > 2 else vmem((hl,), BF16),
        vmem((n_par, hl), F32),
        vmem((hidden, lat), BF16),
        vmem((hidden, lat), BF16),
        vmem((STEPS, half, lat), F32),
        vmem((sections, half, hidden), F32),
        vmem((sections, half, hidden), BF16),
        vmem((sections, half, hidden), BF16),
        vmem((sections, lat, half), BF16),
        vmem((sections, lat, half), BF16),
        vmem((others, plan.chunks, lat, plan.cols), BF16),
        vmem((others, plan.chunks, lat, plan.cols), BF16),
        dma((2, others, 3)),
        dma((2, others, plan.chunks)),
        dma((2, others)),
    ]
    grad_rows = plan.piece if plan.scatter else lat
    if plan.scatter:
        scratch.append(dma((2, plan.messages)))
        tail = (plan.piece, plan.cols)
        for chunk in range(plan.chunks):
            for stage, group in enumerate(plan.orders[chunk]):
                here = (2,) * len(plan.left(chunk, stage)) + tail
                after = (2,) * len(plan.left(chunk, stage + 1)) + tail
                scratch.append(vmem(here, F32))
                scratch.append(vmem(here, BF16))
                scratch.append(vmem(((1 << len(group)) - 1,) + after, BF16))
    in_vmem = pl.BlockSpec(memory_space=pltpu.VMEM)
    anywhere = pl.BlockSpec(memory_space=pl.ANY)
    back, grad_in, grad_out = pl.pallas_call(
        functools.partial(kernel, plan),
        name="adjoint",
        out_shape=(
            jax.ShapeDtypeStruct((rows, lat), F32),
            jax.ShapeDtypeStruct((grad_rows, hl), F32),
            jax.ShapeDtypeStruct((grad_rows, hl), F32),
        ),
        in_specs=[anywhere] * 9,
        out_specs=(in_vmem,) * 3,
        scratch_shapes=scratch,
        compiler_params=pltpu.CompilerParams(
            collective_id=0,
            has_side_effects=True,
            vmem_limit_bytes=60 * 1024 * 1024,
        ),
    )(
        states,
        cotangent,
        obs_count,
        step_index,
        step_table,
        w_in,
        b_hid,
        w_out,
        b_out[None, :],
    )
    if not plan.scatter:
        grad_in, grad_out = (
            lax.psum_scatter(grad, "seq", scatter_dimension=0, tiled=True)
            for grad in (grad_in, grad_out)
        )
    return (back, grad_in, grad_out)


def solution(mesh):
    return jax.shard_map(
        per_device,
        mesh=mesh,
        in_specs=(
            P("seq", None),
            P("seq", None),
            P("seq"),
            P(None, "seq"),
            P(),
            P(None, "par"),
            P("par"),
            P(None, "par"),
            P(),
        ),
        out_specs=(P("seq", None), P("seq", "par"), P("seq", "par")),
        check_vma=False,
    )
```
